256 devices in a mesh: slab: 128 (over x, z, y), pencil: 2 (over core).
Axes of the slice: x: 4, y: 4, z: 8, core: 2. Of those that a mesh axis runs over, the one named last changes fastest.
Arguments:
- density: float32 [768, 768, 384], P('slab', 'pencil'), may hold values from 0 to 1
- cell_kind: int32 [768, 768, 384], P('slab', 'pencil'), may hold values from 0 to 2
- sharpness: float32 [1], replicated, may hold values from 48 to 96
- fraction: float32 [1], replicated, may hold values from 0.36 to 0.41
Outputs:
- physical: float32 [768, 768, 384], P('slab', 'pencil')
- threshold: float32 [1], replicated
The draws below stay inside these ranges and needn't reach their ends.
Inputs may be any that keep to these rules, and one draw needn't show every extreme that they name: `cell_kind`: each cell is a design, void or solid cell.
All inputs are finite; a program needn't handle non-finite values.
Results may differ from the reference program's by a relative error of at most 0.0003.
Values sent between devices are 32-bit elements; how exact they have to be, the bound alone decides.
A program may use at most 128 MiB of HBM per device.

```python
import math
import jax
import jax.numpy as jnp
from jax import lax

RADIUS = 5
ITERS = 3
NZ = 768
NY = 768
NX = 384


def draw_density(key, part):
    wave_draw = jax.random.uniform(jax.random.fold_in(key, 11), (6, 3), jnp.float32)
    sign_flip = jnp.where(jax.random.bernoulli(jax.random.fold_in(key, 12), 0.5, (6, 3)), 1.0, -1.0)
    phase_shift = jax.random.uniform(jax.random.fold_in(key, 13), (6,), jnp.float32, -math.pi, math.pi)
    cycles = sign_flip / (24.0 * jnp.power(4.0, wave_draw))
    depth_axis = jnp.arange(NZ, dtype=jnp.float32)[:, None, None]
    row_axis = jnp.arange(NY, dtype=jnp.float32)[None, :, None]
    column_axis = jnp.arange(NX, dtype=jnp.float32)[None, None, :]
    pattern = jnp.zeros((NZ, NY, NX), jnp.float32)
    for component in range(6):
        argument = cycles[component, 0] * depth_axis + cycles[component, 1] * row_axis + cycles[component, 2] * column_axis
        pattern = pattern + jnp.cos(2.0 * math.pi * argument + phase_shift[component])
    pattern = pattern / math.sqrt(3.0)
    middle_value = 0.62
    amplitude = 0.3
    roughness = 0.2
    jitter = jax.random.uniform(jax.random.fold_in(key, 14), (NZ, NY, NX), jnp.float32, -roughness, roughness)
    return jnp.clip(middle_value + amplitude * pattern + jitter, 0.0, 1.0).astype(jnp.float32)


def set_ends(result, stream_key, low, largest):
    dims = result.shape
    place = [jax.random.randint(jax.random.fold_in(stream_key, axis), (), 0, dims[axis]) for axis in range(len(dims))]
    result = result.at[tuple(place)].set(low)
    longest = dims.index(max(dims))
    place[longest] = (place[longest] + 1) % dims[longest]
    return result.at[tuple(place)].set(largest)


def setup_inputs(seed: int = 0) -> dict:
    key_list = jax.random.split(jax.random.key(seed), 5)
    density = draw_density(jax.random.fold_in(key_list[4], 71), 0)
    cell_kind = set_ends(jax.random.randint(key_list[1], (NZ, NY, NX), 0, 3), jax.random.fold_in(key_list[1], 1), 0, 2).astype(jnp.int32)
    sharpness = jnp.clip(jnp.exp(jax.random.uniform(key_list[2], (1,), jnp.float32, math.log(48.0), math.log(96.0))), 48.0, 96.0)
    fraction = jnp.clip(jax.random.uniform(key_list[3], (1,), jnp.float32, 0.36, 0.41), 0.36, 0.41)
    return dict(density=density, cell_kind=cell_kind, sharpness=sharpness, fraction=fraction)


def smooth_axis(field, axis):
    length = field.shape[axis]
    pads = [(0, 0), (0, 0), (0, 0)]
    pads[axis] = (RADIUS, RADIUS)
    padded = jnp.pad(field, pads)
    total = jnp.zeros_like(field)
    for offset in range(-RADIUS, RADIUS + 1):
        weight = float(RADIUS + 1 - abs(offset))
        piece = lax.slice_in_dim(padded, RADIUS + offset, RADIUS + offset + length, axis=axis)
        total = total + weight * piece
    return total


def coverage(count):
    index = jnp.arange(count, dtype=jnp.int32)
    total = jnp.zeros((count,), jnp.float32)
    for offset in range(-RADIUS, RADIUS + 1):
        inside = ((index + offset >= 0) & (index + offset < count)).astype(jnp.float32)
        total = total + float(RADIUS + 1 - abs(offset)) * inside
    return total


def project(filtered, cell_kind, beta, level):
    tangent = jnp.tanh(beta * (filtered - level))
    design = cell_kind == 0
    solid = cell_kind == 2
    values = jnp.where(design, 0.5 * (1.0 + tangent), jnp.where(solid, 1.0, 0.0))
    return values, tangent, design


def reference(density, cell_kind, sharpness, fraction):
    smoothed = smooth_axis(smooth_axis(smooth_axis(density, 0), 1), 2)
    cover = coverage(NZ)[:, None, None] * coverage(NY)[None, :, None] * coverage(NX)[None, None, :]
    filtered = smoothed / cover
    beta = sharpness[0]
    cells = jnp.float32(NZ * NY * NX)
    level = jnp.float32(0.5)
    for step in range(ITERS):
        values, tangent, design = project(filtered, cell_kind, beta, level)
        volume = jnp.sum(values)
        slope = cells + jnp.sum(jnp.where(design, 0.5 * beta * (1.0 - tangent * tangent), 0.0))
        level = level + (volume - fraction[0] * cells) / slope
    values, tangent, design = project(filtered, cell_kind, beta, level)
    return values, jnp.reshape(level, (1,)).astype(jnp.float32)
```

```python
import functools

import jax
import jax.numpy as jnp
from jax import lax
from jax.experimental import pallas as pl
from jax.experimental.pallas import tpu as pltpu
from jax.sharding import PartitionSpec as P

RADIUS = 5
ITERS = 3
LANES = 128
MESH = pl.DeviceIdType.MESH
FAR = 1e30

CHUNK = 24

NXC, NZC, NYC = 4, 8, 4


def torus_distance(d, n):
    return min(d, n - d)


PLANE = sorted(
    [(dx, dy) for dx in range(NXC) for dy in range(NYC) if (dx, dy) != (0, 0)],
    key=lambda o: -(torus_distance(o[0], NXC) + torus_distance(o[1], NYC)),
)
COLUMN = sorted(
    [(dz, dc) for dz in range(NZC) for dc in range(2) if (dz, dc) != (0, 0)],
    key=lambda o: -torus_distance(o[0], NZC),
)


def coverage_of(index, whole):
    low = jnp.maximum(float(RADIUS) - index, 0.0)
    high = jnp.maximum(index - float(whole - 1 - RADIUS), 0.0)
    full = float((RADIUS + 1) ** 2)
    return full - 0.5 * low * (low + 1.0) - 0.5 * high * (high + 1.0)


def two_boxes(x, axis):
    n = x.shape[axis]
    two = x + pltpu.roll(x, n - 1, axis)
    four = two + pltpu.roll(two, n - 2, axis)
    six = four + pltpu.roll(two, n - 4, axis)
    two = six + pltpu.roll(six, 1, axis)
    four = two + pltpu.roll(two, 2, axis)
    return four + pltpu.roll(two, 4, axis)


def filter_layers(v):
    before, own, after = v[:5], v[5:11], v[11:]
    suffix = [None] * 5
    suffix[4] = before[4]
    for m in range(3, -1, -1):
        suffix[m] = suffix[m + 1] + before[m]
    part_before = [None] * 6
    part_before[4] = suffix[4]
    for k in range(3, -1, -1):
        part_before[k] = part_before[k + 1] + suffix[k]
    prefix = [after[0]]
    for m in range(1, 5):
        prefix.append(prefix[-1] + after[m])
    part_after = [None] * 6
    part_after[1] = prefix[0]
    for k in range(2, 6):
        part_after[k] = part_after[k - 1] + prefix[k - 1]
    sums = [own[0]]
    for j in range(1, 6):
        sums.append(sums[-1] + own[j])
    total = sums[5]
    centre = [functools.reduce(jnp.add, sums)]
    for k in range(5):
        centre.append(centre[-1] + (total - 2.0 * sums[k]))
    out = []
    for k in range(6):
        value = centre[k]
        if part_before[k] is not None:
            value = value + part_before[k]
        if part_after[k] is not None:
            value = value + part_after[k]
        out.append(value)
    return out


def kernel(
    slabs,
    cells,
    density,
    cell_kind,
    sharpness,
    fraction,
    h_out,
    level_out,
    v,
    zf,
    kind,
    acc,
    part,
    recv_a,
    recv_b,
    send_low,
    send_high,
    recv_low,
    recv_high,
    own_sem,
    kind_sem,
    edge_sem,
    send_a,
    send_b,
    arrive_a,
    arrive_b,
):
    depth, rows, cols = density.shape
    steps = rows // CHUNK
    s = lax.axis_index("slab")
    c = lax.axis_index("pencil")
    cx = s // (NZC * NYC)
    cz = (s // NYC) % NZC
    cy = s % NYC

    def plane_peer(dx, dy):
        return {"slab": (((cx + dx) % NXC) * NZC + cz) * NYC + (cy + dy) % NYC, "pencil": c}

    def column_peer(dz, dc):
        return {"slab": (cx * NZC + (cz + dz) % NZC) * NYC + cy, "pencil": (c + dc) % 2}

    up, down = {"slab": s + 1, "pencil": c}, {"slab": s - 1, "pencil": c}
    has_up, has_down = s < slabs - 1, s > 0

    own_copy = pltpu.make_async_copy(density, v.at[5:11], own_sem)
    kind_copy = pltpu.make_async_copy(cell_kind, kind, kind_sem)
    own_copy.start()
    kind_copy.start()

    barrier = pltpu.get_barrier_semaphore()

    @pl.when(has_up)
    def _():
        pl.semaphore_signal(barrier, inc=1, device_id=up, device_id_type=MESH)

    @pl.when(has_down)
    def _():
        pl.semaphore_signal(barrier, inc=1, device_id=down, device_id_type=MESH)

    for offset in COLUMN:
        pl.semaphore_signal(barrier, inc=1, device_id=column_peer(*offset), device_id_type=MESH)
    for offset in PLANE:
        pl.semaphore_signal(barrier, inc=1, device_id=plane_peer(*offset), device_id_type=MESH)

    pl.semaphore_wait(barrier, len(COLUMN) + len(PLANE) + jnp.minimum(s, 1) + jnp.minimum(slabs - 1 - s, 1))

    def first_row(step):
        return pl.multiple_of(jnp.where(c == 1, step, steps - 1 - step) * CHUNK, 8)

    def upward(step):
        part_rows = pl.ds(first_row(step), CHUNK)
        return pltpu.make_async_remote_copy(
            src_ref=density.at[1:6, part_rows, :],
            dst_ref=v.at[0:5, part_rows, :],
            send_sem=send_low,
            recv_sem=recv_low.at[step],
            device_id=up,
            device_id_type=MESH,
        )

    def downward(step):
        part_rows = pl.ds(first_row(step), CHUNK)
        return pltpu.make_async_remote_copy(
            src_ref=density.at[0:5, part_rows, :],
            dst_ref=v.at[11:16, part_rows, :],
            send_sem=send_high,
            recv_sem=recv_high.at[step],
            device_id=down,
            device_id_type=MESH,
        )

    def send(step, carry):
        @pl.when(has_up)
        def _():
            upward(step).start()

        @pl.when(has_down)
        def _():
            downward(step).start()

        return carry

    lax.fori_loop(0, steps, send, 0)

    @pl.when(jnp.logical_not(has_down))
    def _():
        v[0:5] = jnp.zeros((5, rows, cols), jnp.float32)

    @pl.when(jnp.logical_not(has_up))
    def _():
        v[11:16] = jnp.zeros((5, rows, cols), jnp.float32)

    outer = pl.multiple_of(jnp.where(c == 0, 0, rows + 8), 8)
    zf[:, pl.ds(outer, 8), :] = jnp.zeros((depth, 8, cols), jnp.float32)
    acc[...] = jnp.zeros_like(acc)

    beta = sharpness[0]
    lane = lax.broadcasted_iota(jnp.int32, (1, cols), 1).astype(jnp.float32)
    over_x = 1.0 / coverage_of(lane, cols)

    edge_from = pl.multiple_of(jnp.where(c == 0, rows, 8), 8)
    edge = pltpu.make_async_remote_copy(
        src_ref=zf.at[:, pl.ds(edge_from, 8), :],
        dst_ref=zf.at[:, pl.ds(pl.multiple_of(jnp.where(c == 0, 0, rows + 8), 8), 8), :],
        send_sem=edge_sem.at[0],
        recv_sem=edge_sem.at[1],
        device_id={"slab": s, "pencil": 1 - c},
        device_id_type=MESH,
    )

    def along_z(step):
        start = first_row(step)
        for group in range(CHUNK // 8):
            at = pl.ds(pl.multiple_of(start + group * 8, 8), 8)
            to = pl.ds(pl.multiple_of(start + group * 8 + 8, 8), 8)
            for tile in range(cols // LANES):
                lanes = slice(tile * LANES, (tile + 1) * LANES)
                filtered = filter_layers([v[m, at, lanes] for m in range(16)])
                for k in range(depth):
                    zf[k, to, lanes] = filtered[k]

    def along_y_x(step):
        start = first_row(step)
        row = (c * rows + start + lax.broadcasted_iota(jnp.int32, (CHUNK, 1), 0)).astype(jnp.float32)
        scale = (beta / coverage_of(row, 2 * rows)) * over_x

        def layer(k, carry):
            block = zf[k, pl.ds(start, CHUNK + 16), :]
            y = two_boxes(block, 0)[8 : 8 + CHUNK]
            wide = jnp.concatenate([y, jnp.zeros((CHUNK, LANES), jnp.float32)], axis=1)
            x = two_boxes(wide, 1)[:, :cols]
            over_z = 1.0 / coverage_of(jnp.full((1, 1), s * depth + k, jnp.int32).astype(jnp.float32), depth * slabs)
            h = x * (scale * over_z)
            which = kind[k, pl.ds(start, CHUNK), :]
            h = jnp.where(which == 0, h, jnp.where(which == 2, FAR, -FAR))
            h_out[k, pl.ds(start, CHUNK), :] = h
            t = jnp.tanh(h - 0.5 * beta)
            q = 1.0 - t * t
            for group in range(CHUNK // 8):
                piece = slice(group * 8, group * 8 + 8)
                acc[0] += t[piece]
                acc[1] += q[piece]
            return carry

        lax.fori_loop(0, depth, layer, 0)

    own_copy.wait()

    def walk(step, carry):
        @pl.when(step == 1)
        def _():
            edge.start()

        @pl.when(has_down)
        def _():
            upward(step).wait_recv()

        @pl.when(has_up)
        def _():
            downward(step).wait_recv()

        along_z(step)

        @pl.when(step == 1)
        def _():
            edge.wait()
            kind_copy.wait()

        @pl.when(step >= 1)
        def _():
            along_y_x(step - 1)

        return carry

    lax.fori_loop(0, steps, walk, 0)
    along_y_x(steps - 1)

    def fold(x):
        total = x[:, :LANES]
        for tile in range(1, cols // LANES):
            total = total + x[:, tile * LANES : (tile + 1) * LANES]
        return jnp.sum(total, axis=0, keepdims=True)

    peers_a = [plane_peer(*offset) for offset in PLANE]
    peers_b = [column_peer(*offset) for offset in COLUMN]
    lane_index = lax.broadcasted_iota(jnp.int32, (1, LANES), 1)

    def copy_a(it, j):
        return pltpu.make_async_remote_copy(
            src_ref=part.at[it, 0],
            dst_ref=recv_a.at[it, j],
            send_sem=send_a.at[it],
            recv_sem=arrive_a.at[it],
            device_id=peers_a[j],
            device_id_type=MESH,
        )

    def copy_b(it, j):
        return pltpu.make_async_remote_copy(
            src_ref=part.at[it, 1],
            dst_ref=recv_b.at[it, j],
            send_sem=send_b.at[it],
            recv_sem=arrive_b.at[it],
            device_id=peers_b[j],
            device_id_type=MESH,
        )

    def everywhere(it, sums_t, sums_q):
        mine = jnp.where(
            lane_index == 0,
            jnp.sum(sums_t, axis=1, keepdims=True),
            jnp.where(lane_index == 1, jnp.sum(sums_q, axis=1, keepdims=True), 0.0),
        )
        part[it, 0] = mine
        for j in range(len(PLANE)):
            copy_a(it, j).start()
        pltpu.make_async_copy(recv_a.at[it], recv_a.at[it], arrive_a.at[it]).wait()
        for j in range(len(PLANE)):
            mine = mine + recv_a[it, j]
        part[it, 1] = mine
        for j in range(len(COLUMN)):
            copy_b(it, j).start()
        pltpu.make_async_copy(recv_b.at[it], recv_b.at[it], arrive_b.at[it]).wait()
        for j in range(len(COLUMN)):
            mine = mine + recv_b[it, j]
        return (
            jnp.sum(jnp.where(lane_index == 0, mine, 0.0), axis=1, keepdims=True),
            jnp.sum(jnp.where(lane_index == 1, mine, 0.0), axis=1, keepdims=True),
        )

    def next_level(it, level, sums_t, sums_q):
        sum_t, sum_q = everywhere(it, sums_t, sums_q)
        volume = 0.5 * (cells + sum_t)
        slope = cells + (0.5 * beta) * sum_q
        return level + (volume - fraction[0] * cells) / slope

    def sums_at(level):
        shift = jnp.broadcast_to(beta * level, (8, cols))

        def rows_of(r, carry):
            sum_t, sum_q = carry
            at = pl.ds(pl.multiple_of(r * 8, 8), 8)
            for k in range(depth):
                t = jnp.tanh(h_out[k, at, :] - shift)
                sum_t = sum_t + t
                sum_q = sum_q + (1.0 - t * t)
            return (sum_t, sum_q)

        zero = jnp.zeros((8, cols), jnp.float32)
        sum_t, sum_q = lax.fori_loop(0, rows // 8, rows_of, (zero, zero))
        return (fold(sum_t), fold(sum_q))

    level = next_level(0, jnp.full((1, 1), 0.5, jnp.float32), fold(acc[0]), fold(acc[1]))

    def newton(it, level):
        return next_level(it, level, *sums_at(level))

    level = lax.fori_loop(1, ITERS, newton, level)
    level_out[...] = jnp.broadcast_to(level, (8, LANES))

    @pl.when(has_up)
    def _():
        pltpu.make_async_copy(density.at[1:6], v.at[0:5], send_low).wait()

    @pl.when(has_down)
    def _():
        pltpu.make_async_copy(density.at[0:5], v.at[11:16], send_high).wait()

    for it in range(ITERS):
        pltpu.make_async_copy(recv_a.at[it], recv_a.at[it], send_a.at[it]).wait()
        pltpu.make_async_copy(recv_b.at[it], recv_b.at[it], send_b.at[it]).wait()


def local(slabs, pencils, density, cell_kind, sharpness, fraction):
    depth, rows, cols = density.shape
    steps = rows // CHUNK
    cells = float(depth * slabs * rows * pencils * cols)
    na, nb = len(PLANE), len(COLUMN)
    h, level = pl.pallas_call(
        functools.partial(kernel, slabs, cells),
        out_shape=(
            jax.ShapeDtypeStruct((depth, rows, cols), jnp.float32),
            jax.ShapeDtypeStruct((8, LANES), jnp.float32),
        ),
        in_specs=[
            pl.BlockSpec(memory_space=pl.ANY),
            pl.BlockSpec(memory_space=pl.ANY),
            pl.BlockSpec(memory_space=pltpu.SMEM),
            pl.BlockSpec(memory_space=pltpu.SMEM),
        ],
        out_specs=(
            pl.BlockSpec(memory_space=pltpu.VMEM),
            pl.BlockSpec(memory_space=pltpu.VMEM),
        ),
        scratch_shapes=[
            pltpu.VMEM((16, rows, cols), jnp.float32),
            pltpu.VMEM((depth, rows + 16, cols), jnp.float32),
            pltpu.VMEM((depth, rows, cols), jnp.int32),
            pltpu.VMEM((2, 8, cols), jnp.float32),
            pltpu.VMEM((ITERS, 2, 1, LANES), jnp.float32),
            pltpu.VMEM((ITERS, na, 1, LANES), jnp.float32),
            pltpu.VMEM((ITERS, nb, 1, LANES), jnp.float32),
            pltpu.SemaphoreType.DMA,
            pltpu.SemaphoreType.DMA,
            pltpu.SemaphoreType.DMA((steps,)),
            pltpu.SemaphoreType.DMA((steps,)),
            pltpu.SemaphoreType.DMA,
            pltpu.SemaphoreType.DMA,
            pltpu.SemaphoreType.DMA((2,)),
            pltpu.SemaphoreType.DMA((ITERS,)),
            pltpu.SemaphoreType.DMA((ITERS,)),
            pltpu.SemaphoreType.DMA((ITERS,)),
            pltpu.SemaphoreType.DMA((ITERS,)),
        ],
        compiler_params=pltpu.CompilerParams(
            collective_id=0, has_side_effects=True, vmem_limit_bytes=48 * 1024 * 1024
        ),
        name="filter_and_newton",
    )(density, cell_kind, sharpness, fraction)
    level = level[0, :1]
    values = 0.5 * (1.0 + jnp.tanh(h - sharpness[0] * level[0]))
    return (values, level)


def solution(mesh):
    return jax.shard_map(
        functools.partial(local, mesh.shape["slab"], mesh.shape["pencil"]),
        mesh=mesh,
        in_specs=(P("slab", "pencil", None), P("slab", "pencil", None), P(), P()),
        out_specs=(P("slab", "pencil", None), P()),
        check_vma=False,
    )
```
